32 devices in a mesh: seq: 8 (over z, y), head: 4 (over x, core).
Axes of the slice: x: 2, y: 2, z: 4, core: 2. Of those that a mesh axis runs over, the one named last changes fastest.
Arguments:
- q_nope: bfloat16 [4, 64, 128], P(None, 'head'), may hold values from -5 to 5
- q_rope: bfloat16 [4, 64, 64], P(None, 'head'), may hold values from -16 to 16
- w_key_up: bfloat16 [64, 128, 512], P('head'), may hold values from -0.5 to 0.5
- w_value_up: bfloat16 [64, 512, 128], P('head'), may hold values from -0.25 to 0.25
- latent_cache: bfloat16 [512, 64, 576], P('seq'), may hold values from -34 to 34
- page_scale: float32 [512], P('seq'), may hold values from 0.25 to 2, as said below
- block_table: int32 [4, 128], P(None, 'seq'), may hold values from 0 to 63, as said below
- lengths: int32 [4], replicated, may hold values from 1 to 8192, 20480 in all
Outputs:
- attn_out: bfloat16 [4, 8192], P('head', 'seq')
The draws below stay inside these ranges and needn't reach their ends.
Inputs may be any that keep to these rules, and one draw needn't show every extreme that they name: `block_table`: each entry is the number of a page within its pool; for each index of seq, the entries of its 16 page columns over all requests name every page of its pool exactly once. `page_scale`: every page scale is positive. `lengths`: each request has at least one cached position and at most 8192; the longest has exactly 8192.
All inputs are finite; a program needn't handle non-finite values.
Results may differ from the reference program's by a relative error of at most 0.0095.
Values may be sent and summed in bfloat16 or wider, within the bound.
A program may use at most 64 MiB of HBM per device.

```python
import math
import jax
import jax.numpy as jnp
import numpy as np
from jax import lax

LAT = 512
ROPE = 64
NOPE = 128
VDIM = 128
HEADS = 64
PAGE = 64
BATCH = 4
BLOCKS_DEV = 16
PAGES_DEV = 64
CTX = 8192
BLOCKS = 128
PAGES = 512


def page_scales(key):
    base = jax.random.fold_in(key, 11)
    uniform_draw = jax.random.uniform(base, (PAGES,), jnp.float32)
    scales = jnp.exp(jnp.log(0.5) + uniform_draw * jnp.log(2.0))
    return scales


def rope_signs(key):
    picker = jax.random.uniform(jax.random.fold_in(key, 37), (ROPE,), jnp.float32)
    return jnp.where(picker < 0.5, -1.0, 1.0).astype(jnp.float32)


def draw_page_scale(key, part):
    return page_scales(key).astype(jnp.float32)


def draw_block_table(key, part):
    groups = BLOCKS // BLOCKS_DEV
    subkeys = jax.random.split(key, groups)
    orders = jax.vmap(lambda single: jax.random.permutation(single, PAGES_DEV))(subkeys)
    mapping = orders.reshape(groups, BATCH, BLOCKS_DEV).transpose(1, 0, 2).reshape(BATCH, BLOCKS)
    return mapping.astype(jnp.int32)


def draw_q_rope(key, part):
    base = jax.random.fold_in(key, 41)
    plain = jnp.clip(jax.random.normal(base, (BATCH, HEADS, ROPE), jnp.float32), -5.0, 5.0)
    jitter = jnp.clip(jax.random.normal(jax.random.fold_in(base, 1), (HEADS, ROPE), jnp.float32), -1.0, 1.0)
    aligned = 15.0 * rope_signs(key)[None, :] + jitter
    first_row = (jnp.arange(BATCH, dtype=jnp.int32) == 0)[:, None, None]
    return jnp.where(first_row, aligned[None, :, :], plain).astype(jnp.bfloat16)


def draw_latent_cache(key, part):
    width = LAT + ROPE
    base = jax.random.fold_in(key, 23)
    amp_key, dir_key, noise_key = jax.random.split(base, 3)
    amp_draw = jax.random.uniform(amp_key, (PAGES, 1, 1), jnp.float32)
    amplitude = jnp.exp(jnp.log(0.25) + amp_draw * jnp.log(6.0))
    scales = page_scales(key)
    direction = jnp.clip(jax.random.normal(dir_key, (PAGES, 1, width), jnp.float32), -4.0, 4.0)
    noise = jnp.clip(jax.random.normal(noise_key, (PAGES, PAGE, width), jnp.float32), -4.0, 4.0)
    stored = amplitude * direction + noise
    table = draw_block_table(key, part)
    first_ids = jnp.arange(BLOCKS, dtype=jnp.int32) // BLOCKS_DEV * PAGES_DEV + table[0]
    marked = jnp.zeros((PAGES,), jnp.float32).at[first_ids].set(1.0)
    rope_key = 7.0 * rope_signs(key)[None, None, :] / scales[:, None, None] + noise[:, :, LAT:]
    rope_part = jnp.where(marked[:, None, None] > 0.5, rope_key, stored[:, :, LAT:])
    stored = jnp.concatenate([stored[:, :, :LAT], rope_part], axis=2)
    return stored.astype(jnp.bfloat16)


def level_of(stream_key, extent, pieces, least, largest):
    gain, own = 1.0, jax.random.fold_in(stream_key, 6)
    for position, parts in pieces:
        draws = jnp.exp(jax.random.uniform(jax.random.fold_in(own, position), (parts,), jnp.float32, least / len(pieces), largest / len(pieces)))
        gain = gain * jnp.repeat(draws, extent[position] // parts).reshape([-1 if axis == position else 1 for axis in range(len(extent))])
    return gain


def split_up(amount, total, limit, skew):
    loads = [(1 << 20) // math.isqrt(rank ** skew) + 1 for rank in range(2, amount + 1)]
    surplus, given = total - limit - (amount - 1), [1] * (amount - 1)
    while surplus > 0:
        candidates = [i for i in range(amount - 1) if given[i] < limit]
        pool, left = sum([loads[i] for i in candidates]), surplus
        for i in candidates:
            addition = min(limit - given[i], max(1, left * loads[i] // pool), surplus)
            given[i] = given[i] + addition
            surplus = surplus - addition
    return np.array([limit] + given)


def uneven_parts(stream_key, count, total, reach, slope):
    if count == 2:
        one = jax.random.randint(stream_key, (), max(1, total - reach), min(reach, total - 1) + 1)
        return jnp.stack([one, total - one])
    sizes = jnp.asarray(split_up(count, total, reach, slope), jnp.int32)
    couples = (count - 1) // 2
    source_of, sink = sizes[1:1 + 2 * couples:2], sizes[2:2 + 2 * couples:2]
    margin = jnp.minimum(source_of - 1, reach - sink)
    moved = jax.random.randint(jax.random.fold_in(stream_key, 1), (couples,), 0, 1 << 20) % (margin + 1)
    sizes = sizes.at[1:1 + 2 * couples:2].set(source_of - moved).at[2:2 + 2 * couples:2].set(sink + moved)
    return sizes[jax.random.permutation(jax.random.fold_in(stream_key, 2), count)]


def gaussian(rng, dims, scale, bound, shards=(), kind=jnp.bfloat16):
    values = jax.random.normal(rng, dims, jnp.float32) * scale
    if len(shards) > 0:
        values = level_of(rng, dims, shards, -0.22, 0.18) * values
    return jnp.clip(values, min=-bound, max=bound).astype(kind)


def setup_inputs(seed: int = 0) -> dict:
    seeds = jax.random.split(jax.random.key(seed), 9)
    return {
        "q_nope": gaussian(seeds[0], (BATCH, HEADS, NOPE), 1.0, 5.0, ((1, 4),)),
        "q_rope": draw_q_rope(jax.random.fold_in(seeds[8], 71), 0),
        "w_key_up": gaussian(seeds[2], (HEADS, NOPE, LAT), NOPE ** -0.5, 0.5, ((0, 4),)),
        "w_value_up": gaussian(seeds[3], (HEADS, LAT, VDIM), LAT ** -0.5, 0.25, ((0, 4),)),
        "latent_cache": draw_latent_cache(jax.random.fold_in(seeds[8], 71), 0),
        "page_scale": draw_page_scale(jax.random.fold_in(seeds[8], 71), 0),
        "block_table": draw_block_table(jax.random.fold_in(seeds[8], 71), 0),
        "lengths": uneven_parts(seeds[7], BATCH, 5 * BATCH * CTX // 8, CTX, 0).astype(jnp.int32),
    }


floor_score = -1e30


def reference(q_nope, q_rope, w_key_up, w_value_up, latent_cache, page_scale, block_table, lengths):
    softmax_scale = (NOPE + ROPE) ** -0.5
    q_latent = jnp.einsum("bhn,hnl->bhl", q_nope.astype(jnp.float32), w_key_up.astype(jnp.float32)).astype(jnp.bfloat16)

    def attend(request):
        page_ids = (jnp.arange(BLOCKS, dtype=jnp.int32) // BLOCKS_DEV) * PAGES_DEV + block_table[request]
        cache_rows = latent_cache[page_ids].reshape(CTX, LAT + ROPE)
        scale_rows = jnp.repeat(page_scale[page_ids], PAGE)
        raw_scores = jnp.dot(q_latent[request], cache_rows[:, :LAT].T, preferred_element_type=jnp.float32)
        raw_scores = raw_scores + jnp.dot(q_rope[request], cache_rows[:, LAT:].T, preferred_element_type=jnp.float32)
        usable = jnp.arange(CTX, dtype=jnp.int32) < lengths[request]
        scores = jnp.where(usable[None, :], raw_scores * (scale_rows * softmax_scale)[None, :], floor_score)
        maximum = jnp.max(scores, axis=1, keepdims=True)
        weights = jnp.where(usable[None, :], jnp.exp(scores - maximum), 0.0)
        denominator = jnp.sum(weights, axis=1)
        probabilities = (weights * scale_rows[None, :]).astype(jnp.bfloat16)
        weighted = jnp.dot(probabilities, cache_rows[:, :LAT], preferred_element_type=jnp.float32)
        return weighted / denominator[:, None]

    latent_out = lax.map(attend, jnp.arange(BATCH, dtype=jnp.int32))
    projected = jnp.einsum("bhl,hlv->bhv", latent_out, w_value_up.astype(jnp.float32), precision=lax.Precision.HIGHEST)
    return projected.reshape(BATCH, HEADS * VDIM).astype(jnp.bfloat16)
```

```python
import functools

import jax
import jax.numpy as jnp
from jax import lax
from jax.experimental import pallas as pl
from jax.experimental.pallas import tpu as pltpu
from jax.sharding import PartitionSpec as P

floor_score = -1e30
floor_peak = -1e29
LANES = 128
CHUNKS = 4
WK_PARTS = 4
MESH = pl.DeviceIdType.MESH


def loop(count, body):
    if count <= 16:
        for i in range(count):
            body(i)
    else:
        def step(i, carry):
            body(i)
            return carry
        lax.fori_loop(0, count, step, 0)


def kernel(
    n_seq, n_head, width,
    qn_hbm, qr_hbm, wk_hbm, wv_hbm, kv_hbm, scale_hbm, table_hbm, len_ref,
    out_ref,
    qn, qr, wk, wv, kv, scale, table,
    msg, stat, acc_in, stat_in, mix,
    small_sem, wk_sem, kv_sem, wv_sem, send_sem, recv_sem,
):
    batch, heads, nope = qn.shape
    rope = qr.shape[2]
    lat, vdim = wv.shape[1], wv.shape[2]
    pages, page_len, _ = kv.shape
    window = table.shape[1]
    rows = batch * heads
    per_msg = msg.shape[1]
    per_shard = n_seq // n_head
    softmax_scale = (nope + rope) ** (-0.5)
    my_seq = lax.axis_index("seq")
    my_head = lax.axis_index("head")

    small = [
        pltpu.make_async_copy(src, dst, small_sem.at[i])
        for i, (src, dst) in enumerate(
            ((qn_hbm, qn), (qr_hbm, qr), (scale_hbm, scale), (table_hbm, table))
        )
    ]
    for copy in small:
        copy.start()
    wk_step = heads // WK_PARTS
    wk_copies = [
        pltpu.make_async_copy(
            wk_hbm.at[pl.ds(i * wk_step, wk_step)], wk.at[pl.ds(i * wk_step, wk_step)], wk_sem.at[i]
        )
        for i in range(WK_PARTS)
    ]
    for copy in wk_copies:
        copy.start()
    kv_step = pages // CHUNKS
    kv_copies = [
        pltpu.make_async_copy(
            kv_hbm.at[pl.ds(i * kv_step, kv_step)], kv.at[pl.ds(i * kv_step, kv_step)], kv_sem.at[i]
        )
        for i in range(CHUNKS)
    ]
    for copy in kv_copies:
        copy.start()
    wv_copy = pltpu.make_async_copy(wv_hbm, wv, wv_sem.at[0])
    wv_copy.start()

    barrier = pltpu.get_barrier_semaphore()
    source_head = my_seq // per_shard
    own = source_head == my_head

    def greet(i):
        @pl.when(jnp.logical_not(jnp.logical_and(own, i == my_seq)))
        def _():
            pl.semaphore_signal(
                barrier, inc=1, device_id=(jnp.int32(i), source_head), device_id_type=MESH
            )

    loop(n_seq, greet)

    for copy in small:
        copy.wait()

    lane = lax.broadcasted_iota(jnp.int32, (batch, LANES), 1)
    request = lax.broadcasted_iota(jnp.int32, (batch, LANES), 0)
    length = jnp.zeros((batch, LANES), jnp.int32)
    for b in range(batch):
        length = jnp.where(request == b, len_ref[b], length)
    base = my_seq * (window * page_len)
    names = table[...]
    counts = jnp.zeros((batch, LANES), jnp.float32)
    for j in range(window):
        held = jnp.clip(length - (base + j * page_len), 0, page_len).astype(jnp.float32)
        counts = jnp.where(names[:, j : j + 1] == lane, held, counts)
    s_row = scale[...]
    s_hi = s_row.astype(jnp.bfloat16)
    s_rest = s_row - s_hi.astype(jnp.float32)
    s_mid = s_rest.astype(jnp.bfloat16)
    s_low = (s_rest - s_mid.astype(jnp.float32)).astype(jnp.bfloat16)
    per_page = jnp.concatenate(
        [counts[:, :pages]]
        + [s.astype(jnp.float32) for s in (s_hi, s_mid, s_low)]
        + [jnp.zeros((1, pages), jnp.float32)] * (8 - batch - 3),
        axis=0,
    ).astype(jnp.bfloat16)
    positions = pages * page_len
    spread = (
        lax.broadcasted_iota(jnp.int32, (pages, positions), 1) // page_len
        == lax.broadcasted_iota(jnp.int32, (pages, positions), 0)
    ).astype(jnp.float32).astype(jnp.bfloat16)
    per_pos = jnp.dot(per_page, spread, preferred_element_type=jnp.float32)
    scale_pos = per_pos[batch : batch + 1] + per_pos[batch + 1 : batch + 2] + per_pos[batch + 2 : batch + 3]

    query = qn[...].reshape(rows, nope).astype(jnp.float32)
    row_head = lax.broadcasted_iota(jnp.int32, (rows, nope), 0) % heads
    q_lat = jnp.zeros((rows, lat), jnp.float32)
    for i in range(WK_PARTS):
        wide = jnp.concatenate(
            [jnp.where(row_head == h, query, 0.0) for h in range(i * wk_step, (i + 1) * wk_step)],
            axis=1,
        ).astype(jnp.bfloat16)
        wk_copies[i].wait()
        block = wk[pl.ds(i * wk_step, wk_step)].reshape(wk_step * nope, lat)
        q_lat = q_lat + jnp.dot(wide, block, preferred_element_type=jnp.float32)
    q_all = jnp.concatenate([q_lat.astype(jnp.bfloat16), qr[...].reshape(rows, rope)], axis=1)

    span = kv_step * page_len
    offset = (lax.broadcasted_iota(jnp.int32, (1, span), 1) % page_len).astype(jnp.float32)
    parts = []
    for c in range(CHUNKS):
        kv_copies[c].wait()
        block = kv[pl.ds(c * kv_step, kv_step)].reshape(span, lat + rope)
        raw = lax.dot_general(
            q_all, block, (((1,), (1,)), ((), ())), preferred_element_type=jnp.float32
        )
        s_pos = scale_pos[:, c * span : (c + 1) * span]
        score = raw * (s_pos * softmax_scale)
        score = jnp.concatenate(
            [
                jnp.where(
                    jnp.broadcast_to(offset, (heads, span))
                    < jnp.broadcast_to(per_pos[b : b + 1, c * span : (c + 1) * span], (heads, span)),
                    score[b * heads : (b + 1) * heads],
                    floor_score,
                )
                for b in range(batch)
            ],
            axis=0,
        )
        peak = jnp.maximum(jnp.max(score, axis=1, keepdims=True), floor_peak)
        weight = jnp.exp(score - peak)
        total = jnp.sum(weight, axis=1, keepdims=True)
        prob = (weight * s_pos).astype(jnp.bfloat16)
        acc = jnp.dot(prob, block[:, :lat], preferred_element_type=jnp.float32)
        parts.append((peak, total, acc))
    peak = functools.reduce(jnp.maximum, [p[0] for p in parts])
    total = jnp.zeros((rows, 1), jnp.float32)
    acc = jnp.zeros((rows, lat), jnp.float32)
    for p, t, a in parts:
        factor = jnp.exp(p - peak)
        total = total + t * factor
        acc = acc + a * factor

    col = lax.broadcasted_iota(jnp.int32, (rows, LANES), 1)
    pair = jnp.where(col == 0, peak, jnp.where(col == 1, total, 0.0))
    pair = jnp.concatenate([pair, jnp.zeros((LANES - rows, LANES), jnp.float32)], axis=0)
    stat[...] = pair.T[0:2]

    high = acc.astype(jnp.bfloat16)
    low = (acc - high.astype(jnp.float32)).astype(jnp.bfloat16)
    both = jnp.concatenate([high, low], axis=0)
    out_head = lax.broadcasted_iota(jnp.int32, (rows, vdim), 0) % heads
    carried = jnp.zeros((rows, vdim), jnp.float32)
    wv_copy.wait()
    for h in range(0, heads, 2):
        y = jnp.dot(
            both, jnp.concatenate([wv[h], wv[h + 1]], axis=1), preferred_element_type=jnp.float32
        )
        y = y[:rows] + y[rows:]
        carried = jnp.where(out_head == h, y[:, :vdim], carried)
        carried = jnp.where(out_head == h + 1, y[:, vdim:], carried)
    msg[...] = carried.reshape(msg.shape)

    n_dest = per_shard * n_head

    @pl.when(own)
    def _():
        pl.semaphore_wait(barrier, n_dest - 1)

    @pl.when(jnp.logical_not(own))
    def _():
        pl.semaphore_wait(barrier, n_dest)

    def target(k):
        part, request_of = k // n_head, k % n_head
        slot = request_of * (heads // per_msg) + (part * width) // (vdim * per_msg)
        return my_head * per_shard + part, request_of, slot

    def pair_to(k):
        seq_of, head_of, slot = target(k)
        return [
            pltpu.make_async_remote_copy(
                src_ref=src, dst_ref=dst, send_sem=send_sem.at[n, k], recv_sem=recv_sem.at[n, my_seq],
                device_id=(jnp.int32(seq_of), jnp.int32(head_of)), device_id_type=MESH,
            )
            for n, (src, dst) in enumerate(
                ((stat, stat_in.at[my_seq]), (msg.at[slot], acc_in.at[my_seq]))
            )
        ]

    def local_pair(k):
        slot = target(k)[2]
        return [
            pltpu.make_async_copy(src, dst, recv_sem.at[n, my_seq])
            for n, (src, dst) in enumerate(
                ((stat, stat_in.at[my_seq]), (msg.at[slot], acc_in.at[my_seq]))
            )
        ]

    def is_me(k):
        seq_of, head_of, _ = target(k)
        return jnp.logical_and(seq_of == my_seq, head_of == my_head)

    def send(k):
        @pl.when(jnp.logical_not(is_me(k)))
        def _():
            for copy in pair_to(k):
                copy.start()

        @pl.when(is_me(k))
        def _():
            for copy in local_pair(k):
                copy.start()

    loop(n_dest, send)

    def receive(i):
        for n, (src, dst) in enumerate(((stat, stat_in.at[i]), (msg.at[0], acc_in.at[i]))):
            pltpu.make_async_copy(src, dst, recv_sem.at[n, i]).wait()

    loop(n_seq, receive)

    peaks, totals = stat_in[:, 0, :], stat_in[:, 1, :]
    factor = jnp.exp(peaks - jnp.max(peaks, axis=0, keepdims=True))
    denominator = jnp.sum(factor * totals, axis=0, keepdims=True)
    used = lax.broadcasted_iota(jnp.int32, (1, LANES), 1) < rows
    factor = factor / jnp.where(used, denominator, 1.0)
    if n_seq < LANES:
        factor = jnp.concatenate(
            [factor, jnp.zeros((LANES - n_seq, LANES), jnp.float32)], axis=0
        )
    mix[...] = factor.T.reshape(mix.shape)
    first = (my_seq % per_shard) * width
    weights = mix[my_head * (heads // per_msg) + first // (vdim * per_msg)]
    result = jnp.zeros((per_msg, vdim), jnp.float32)
    for i in range(n_seq):
        result = result + weights[:, i : i + 1] * acc_in[i]
    if width >= vdim:
        for r in range(per_msg):
            out_ref[:, r * vdim : (r + 1) * vdim] = result[r : r + 1].astype(out_ref.dtype)
    else:
        picked = result[:, :width]
        for k in range(1, vdim // width):
            here = (my_seq % (vdim // width)) == k
            picked = jnp.where(here, result[:, k * width : (k + 1) * width], picked)
        out_ref[...] = picked.astype(out_ref.dtype)

    def sent(k):
        @pl.when(jnp.logical_not(is_me(k)))
        def _():
            for copy in pair_to(k):
                copy.wait_send()

    loop(n_dest, sent)


def solution(mesh):
    n_seq, n_head = mesh.shape["seq"], mesh.shape["head"]

    def shards(q_nope, q_rope, w_key_up, w_value_up, latent_cache, page_scale, block_table, lengths):
        batch, heads, _ = q_nope.shape
        vdim = w_value_up.shape[2]
        width = heads * n_head * vdim // n_seq
        per_msg = max(1, width // vdim)
        n_dest = (n_seq // n_head) * n_head
        assert batch == n_head and batch * heads <= LANES and n_seq % n_head == 0
        vmem = lambda a: pltpu.VMEM(a.shape, a.dtype)
        scale_row = page_scale.reshape(1, page_scale.shape[0])
        big = (q_nope, q_rope, w_key_up, w_value_up, latent_cache, scale_row, block_table)
        return pl.pallas_call(
            functools.partial(kernel, n_seq, n_head, width),
            out_shape=jax.ShapeDtypeStruct((1, width), jnp.bfloat16),
            in_specs=[pl.BlockSpec(memory_space=pl.ANY)] * 7
            + [pl.BlockSpec(memory_space=pltpu.SMEM)],
            out_specs=pl.BlockSpec(memory_space=pltpu.VMEM),
            scratch_shapes=[vmem(a) for a in big]
            + [
                pltpu.VMEM((batch * heads // per_msg, per_msg, vdim), jnp.float32),
                pltpu.VMEM((2, LANES), jnp.float32),
                pltpu.VMEM((n_seq, per_msg, vdim), jnp.float32),
                pltpu.VMEM((n_seq, 2, LANES), jnp.float32),
                pltpu.VMEM((LANES // per_msg, per_msg, LANES), jnp.float32),
                pltpu.SemaphoreType.DMA((4,)),
                pltpu.SemaphoreType.DMA((WK_PARTS,)),
                pltpu.SemaphoreType.DMA((CHUNKS,)),
                pltpu.SemaphoreType.DMA((1,)),
                pltpu.SemaphoreType.DMA((2, n_dest)),
                pltpu.SemaphoreType.DMA((2, n_seq)),
            ],
            compiler_params=pltpu.CompilerParams(collective_id=0, has_side_effects=True),
        )(*big, lengths)

    in_specs = (
        P(None, "head", None),
        P(None, "head", None),
        P("head", None, None),
        P("head", None, None),
        P("seq", None, None),
        P("seq"),
        P(None, "seq"),
        P(),
    )
    out_specs = P("head", "seq")
    return jax.shard_map(shards, mesh=mesh, in_specs=in_specs, out_specs=out_specs, check_vma=False)
```

```python
import functools

import jax
import jax.numpy as jnp
from jax import lax
from jax.experimental import pallas as pl
from jax.experimental.pallas import tpu as pltpu
from jax.sharding import PartitionSpec as P

floor_score = -1e30
floor_peak = -1e29
LANES = 128
CHUNKS = 4
WV_PARTS = 2
WINDOW = 6
WK_PARTS = 4
MESH = pl.DeviceIdType.MESH


def loop(count, body):
    if count <= 16:
        for i in range(count):
            body(i)
    else:
        def step(i, carry):
            body(i)
            return carry
        lax.fori_loop(0, count, step, 0)


def kernel(
    n_seq, n_head, width,
    qn_hbm, qr_hbm, wk_hbm, wv_hbm, kv_hbm, scale_hbm, table_hbm, len_ref,
    out_ref,
    qn, qr, wk, wv, kv, scale, table,
    msg, stat, acc_in, stat_in, mix,
    small_sem, wk_sem, kv_sem, wv_sem, send_sem, recv_sem,
):
    batch, heads, nope = qn.shape
    rope = qr.shape[2]
    lat, vdim = wv.shape[1], wv.shape[2]
    pages, page_len, _ = kv.shape
    window = table.shape[1]
    rows = batch * heads
    per_msg = msg.shape[1]
    per_shard = n_seq // n_head
    softmax_scale = (nope + rope) ** (-0.5)
    my_seq = lax.axis_index("seq")
    my_head = lax.axis_index("head")

    small = [
        pltpu.make_async_copy(src, dst, small_sem.at[i])
        for i, (src, dst) in enumerate(
            ((qn_hbm, qn), (qr_hbm, qr), (scale_hbm, scale), (table_hbm, table))
        )
    ]
    for copy in small:
        copy.start()
    wk_step, kv_step, wv_step = heads // WK_PARTS, pages // CHUNKS, heads // WV_PARTS

    def piece(src, dst, sem, i, step):
        part = pl.ds(i * step, step)
        return pltpu.make_async_copy(src.at[part], dst.at[part], sem.at[i])

    wk_copies = [piece(wk_hbm, wk, wk_sem, i, wk_step) for i in range(WK_PARTS)]
    kv_copies = [piece(kv_hbm, kv, kv_sem, i, kv_step) for i in range(CHUNKS)]
    wv_copies = [piece(wv_hbm, wv, wv_sem, i, wv_step) for i in range(WV_PARTS)]
    waiting = wk_copies + kv_copies + wv_copies
    for _ in range(WINDOW):
        waiting.pop(0).start()

    def arrive(copy):
        copy.wait()
        if waiting:
            waiting.pop(0).start()

    barrier = pltpu.get_barrier_semaphore()
    source_head = my_seq // per_shard
    own = source_head == my_head

    def greet(i):
        @pl.when(jnp.logical_not(jnp.logical_and(own, i == my_seq)))
        def _():
            pl.semaphore_signal(
                barrier, inc=1, device_id=(jnp.int32(i), source_head), device_id_type=MESH
            )

    loop(n_seq, greet)

    for copy in small:
        copy.wait()

    lane = lax.broadcasted_iota(jnp.int32, (batch, LANES), 1)
    request = lax.broadcasted_iota(jnp.int32, (batch, LANES), 0)
    length = jnp.zeros((batch, LANES), jnp.int32)
    for b in range(batch):
        length = jnp.where(request == b, len_ref[b], length)
    base = my_seq * (window * page_len)
    names = table[...]
    counts = jnp.zeros((batch, LANES), jnp.float32)
    for j in range(window):
        held = jnp.clip(length - (base + j * page_len), 0, page_len).astype(jnp.float32)
        counts = jnp.where(names[:, j : j + 1] == lane, held, counts)
    s_row = scale[...]
    s_hi = s_row.astype(jnp.bfloat16)
    s_rest = s_row - s_hi.astype(jnp.float32)
    s_mid = s_rest.astype(jnp.bfloat16)
    s_low = (s_rest - s_mid.astype(jnp.float32)).astype(jnp.bfloat16)
    per_page = jnp.concatenate(
        [counts[:, :pages]]
        + [s.astype(jnp.float32) for s in (s_hi, s_mid, s_low)]
        + [jnp.zeros((1, pages), jnp.float32)] * (8 - batch - 3),
        axis=0,
    ).astype(jnp.bfloat16)
    positions = pages * page_len
    spread = (
        lax.broadcasted_iota(jnp.int32, (pages, positions), 1) // page_len
        == lax.broadcasted_iota(jnp.int32, (pages, positions), 0)
    ).astype(jnp.float32).astype(jnp.bfloat16)
    per_pos = jnp.dot(per_page, spread, preferred_element_type=jnp.float32)
    scale_pos = per_pos[batch : batch + 1] + per_pos[batch + 1 : batch + 2] + per_pos[batch + 2 : batch + 3]

    query = qn[...].reshape(rows, nope).astype(jnp.float32)
    row_head = lax.broadcasted_iota(jnp.int32, (rows, nope), 0) % heads
    q_lat = jnp.zeros((rows, lat), jnp.float32)
    for i in range(WK_PARTS):
        wide = jnp.concatenate(
            [jnp.where(row_head == h, query, 0.0) for h in range(i * wk_step, (i + 1) * wk_step)],
            axis=1,
        ).astype(jnp.bfloat16)
        arrive(wk_copies[i])
        block = wk[pl.ds(i * wk_step, wk_step)].reshape(wk_step * nope, lat)
        q_lat = q_lat + jnp.dot(wide, block, preferred_element_type=jnp.float32)
    q_all = jnp.concatenate([q_lat.astype(jnp.bfloat16), qr[...].reshape(rows, rope)], axis=1)

    span = kv_step * page_len
    offset = (lax.broadcasted_iota(jnp.int32, (1, span), 1) % page_len).astype(jnp.float32)
    def scores(c):
        arrive(kv_copies[c])
        block = kv[pl.ds(c * kv_step, kv_step)].reshape(span, lat + rope)
        return lax.dot_general(
            q_all, block, (((1,), (1,)), ((), ())), preferred_element_type=jnp.float32
        )

    def attend(c, raw):
        s_pos = scale_pos[:, c * span : (c + 1) * span]
        score = raw * (s_pos * softmax_scale)
        score = jnp.concatenate(
            [
                jnp.where(
                    jnp.broadcast_to(offset, (heads, span))
                    < jnp.broadcast_to(per_pos[b : b + 1, c * span : (c + 1) * span], (heads, span)),
                    score[b * heads : (b + 1) * heads],
                    floor_score,
                )
                for b in range(batch)
            ],
            axis=0,
        )
        peak = jnp.maximum(jnp.max(score, axis=1, keepdims=True), floor_peak)
        weight = jnp.exp(score - peak)
        total = jnp.sum(weight, axis=1, keepdims=True)
        prob = (weight * s_pos).astype(jnp.bfloat16)
        values = kv[pl.ds(c * kv_step, kv_step), :, :lat].reshape(span, lat)
        acc = jnp.dot(prob, values, preferred_element_type=jnp.float32)
        return peak, total, acc

    parts = []
    raw = scores(0)
    for c in range(1, CHUNKS):
        following = scores(c)
        parts.append(attend(c - 1, raw))
        raw = following
    parts.append(attend(CHUNKS - 1, raw))
    peak = functools.reduce(jnp.maximum, [p[0] for p in parts])
    total = jnp.zeros((rows, 1), jnp.float32)
    acc = jnp.zeros((rows, lat), jnp.float32)
    for p, t, a in parts:
        factor = jnp.exp(p - peak)
        total = total + t * factor
        acc = acc + a * factor

    col = lax.broadcasted_iota(jnp.int32, (rows, LANES), 1)
    pair = jnp.where(col == 0, peak, jnp.where(col == 1, total, 0.0))
    pair = jnp.concatenate([pair, jnp.zeros((LANES - rows, LANES), jnp.float32)], axis=0)
    stat[...] = pair.T[0:2]

    high = acc.astype(jnp.bfloat16)
    low = (acc - high.astype(jnp.float32)).astype(jnp.bfloat16)
    both = jnp.concatenate([high, low], axis=0)
    out_head = lax.broadcasted_iota(jnp.int32, (rows, vdim), 0) % heads
    carried = jnp.zeros((rows, vdim), jnp.float32)
    for h in range(0, heads, 2):
        if h % wv_step == 0:
            arrive(wv_copies[h // wv_step])
        y = jnp.dot(
            both, jnp.concatenate([wv[h], wv[h + 1]], axis=1), preferred_element_type=jnp.float32
        )
        y = y[:rows] + y[rows:]
        carried = jnp.where(out_head == h, y[:, :vdim], carried)
        carried = jnp.where(out_head == h + 1, y[:, vdim:], carried)
    msg[...] = carried.reshape(msg.shape)

    n_dest = per_shard * n_head

    @pl.when(own)
    def _():
        pl.semaphore_wait(barrier, n_dest - 1)

    @pl.when(jnp.logical_not(own))
    def _():
        pl.semaphore_wait(barrier, n_dest)

    def target(k):
        part, request_of = k // n_head, k % n_head
        slot = request_of * (heads // per_msg) + (part * width) // (vdim * per_msg)
        return my_head * per_shard + part, request_of, slot

    def pair_to(k):
        seq_of, head_of, slot = target(k)
        return [
            pltpu.make_async_remote_copy(
                src_ref=src, dst_ref=dst, send_sem=send_sem.at[n, k], recv_sem=recv_sem.at[n, my_seq],
                device_id=(jnp.int32(seq_of), jnp.int32(head_of)), device_id_type=MESH,
            )
            for n, (src, dst) in enumerate(
                ((stat, stat_in.at[my_seq]), (msg.at[slot], acc_in.at[my_seq]))
            )
        ]

    def local_pair(k):
        slot = target(k)[2]
        return [
            pltpu.make_async_copy(src, dst, recv_sem.at[n, my_seq])
            for n, (src, dst) in enumerate(
                ((stat, stat_in.at[my_seq]), (msg.at[slot], acc_in.at[my_seq]))
            )
        ]

    def is_me(k):
        seq_of, head_of, _ = target(k)
        return jnp.logical_and(seq_of == my_seq, head_of == my_head)

    def send(k):
        @pl.when(jnp.logical_not(is_me(k)))
        def _():
            for copy in pair_to(k):
                copy.start()

        @pl.when(is_me(k))
        def _():
            for copy in local_pair(k):
                copy.start()

    loop(n_dest, send)

    def receive(i):
        for n, (src, dst) in enumerate(((stat, stat_in.at[i]), (msg.at[0], acc_in.at[i]))):
            pltpu.make_async_copy(src, dst, recv_sem.at[n, i]).wait()

    loop(n_seq, receive)

    peaks, totals = stat_in[:, 0, :], stat_in[:, 1, :]
    factor = jnp.exp(peaks - jnp.max(peaks, axis=0, keepdims=True))
    denominator = jnp.sum(factor * totals, axis=0, keepdims=True)
    used = lax.broadcasted_iota(jnp.int32, (1, LANES), 1) < rows
    factor = factor / jnp.where(used, denominator, 1.0)
    if n_seq < LANES:
        factor = jnp.concatenate(
            [factor, jnp.zeros((LANES - n_seq, LANES), jnp.float32)], axis=0
        )
    mix[...] = factor.T.reshape(mix.shape)
    first = (my_seq % per_shard) * width
    weights = mix[my_head * (heads // per_msg) + first // (vdim * per_msg)]
    result = jnp.zeros((per_msg, vdim), jnp.float32)
    for i in range(n_seq):
        result = result + weights[:, i : i + 1] * acc_in[i]
    if width >= vdim:
        for r in range(per_msg):
            out_ref[:, r * vdim : (r + 1) * vdim] = result[r : r + 1].astype(out_ref.dtype)
    else:
        picked = result[:, :width]
        for k in range(1, vdim // width):
            here = (my_seq % (vdim // width)) == k
            picked = jnp.where(here, result[:, k * width : (k + 1) * width], picked)
        out_ref[...] = picked.astype(out_ref.dtype)

    def sent(k):
        @pl.when(jnp.logical_not(is_me(k)))
        def _():
            for copy in pair_to(k):
                copy.wait_send()

    loop(n_dest, sent)


def solution(mesh):
    n_seq, n_head = mesh.shape["seq"], mesh.shape["head"]

    def shards(q_nope, q_rope, w_key_up, w_value_up, latent_cache, page_scale, block_table, lengths):
        batch, heads, _ = q_nope.shape
        vdim = w_value_up.shape[2]
        width = heads * n_head * vdim // n_seq
        per_msg = max(1, width // vdim)
        n_dest = (n_seq // n_head) * n_head
        assert batch == n_head and batch * heads <= LANES and n_seq % n_head == 0
        vmem = lambda a: pltpu.VMEM(a.shape, a.dtype)
        scale_row = page_scale.reshape(1, page_scale.shape[0])
        big = (q_nope, q_rope, w_key_up, w_value_up, latent_cache, scale_row, block_table)
        return pl.pallas_call(
            functools.partial(kernel, n_seq, n_head, width),
            out_shape=pltpu.VMEM((1, width), jnp.bfloat16),
            in_specs=[pl.BlockSpec(memory_space=pl.ANY)] * 7
            + [pl.BlockSpec(memory_space=pltpu.SMEM)],
            out_specs=pl.BlockSpec(memory_space=pltpu.VMEM),
            scratch_shapes=[vmem(a) for a in big]
            + [
                pltpu.VMEM((batch * heads // per_msg, per_msg, vdim), jnp.float32),
                pltpu.VMEM((2, LANES), jnp.float32),
                pltpu.VMEM((n_seq, per_msg, vdim), jnp.float32),
                pltpu.VMEM((n_seq, 2, LANES), jnp.float32),
                pltpu.VMEM((LANES // per_msg, per_msg, LANES), jnp.float32),
                pltpu.SemaphoreType.DMA((4,)),
                pltpu.SemaphoreType.DMA((WK_PARTS,)),
                pltpu.SemaphoreType.DMA((CHUNKS,)),
                pltpu.SemaphoreType.DMA((WV_PARTS,)),
                pltpu.SemaphoreType.DMA((2, n_dest)),
                pltpu.SemaphoreType.DMA((2, n_seq)),
            ],
            compiler_params=pltpu.CompilerParams(collective_id=0, has_side_effects=True),
        )(*big, lengths)

    in_specs = (
        P(None, "head", None),
        P(None, "head", None),
        P("head", None, None),
        P("head", None, None),
        P("seq", None, None),
        P("seq"),
        P(None, "seq"),
        P(),
    )
    out_specs = P("head", "seq")
    return jax.shard_map(shards, mesh=mesh, in_specs=in_specs, out_specs=out_specs, check_vma=False)
```

```python
import functools

import jax
import jax.numpy as jnp
from jax import lax
from jax.experimental import pallas as pl
from jax.experimental.pallas import tpu as pltpu
from jax.sharding import PartitionSpec as P

floor_score = -1e30
floor_peak = -1e29
LANES = 128
CHUNKS = 4
WV_PARTS = 2
WINDOW = 6
WK_PARTS = 4
MESH = pl.DeviceIdType.MESH


def loop(count, body):
    if count <= 16:
        for i in range(count):
            body(i)
    else:
        def step(i, carry):
            body(i)
            return carry
        lax.fori_loop(0, count, step, 0)


def kernel(
    n_seq, n_head, width,
    qn_hbm, qr_hbm, wk_hbm, wv_hbm, kv_hbm, scale_hbm, table_hbm, len_hbm,
    out_ref,
    qn, qr, wk, wv, kv, scale, table, len_ref,
    msg, stat, acc_in, stat_in, mix,
    small_sem, wk_sem, kv_sem, wv_sem, send_sem, recv_sem,
):
    batch, heads, nope = qn.shape
    rope = qr.shape[2]
    lat, vdim = wv.shape[1], wv.shape[2]
    pages, page_len, _ = kv.shape
    window = table.shape[1]
    rows = batch * heads
    per_msg = msg.shape[1]
    per_shard = n_seq // n_head
    softmax_scale = (nope + rope) ** (-0.5)
    my_seq = lax.axis_index("seq")
    my_head = lax.axis_index("head")

    small = [
        pltpu.make_async_copy(src, dst, small_sem.at[i])
        for i, (src, dst) in enumerate(
            ((qn_hbm, qn), (qr_hbm, qr), (scale_hbm, scale), (table_hbm, table), (len_hbm, len_ref))
        )
    ]
    for copy in small:
        copy.start()
    wk_step, kv_step, wv_step = heads // WK_PARTS, pages // CHUNKS, heads // WV_PARTS

    def piece(src, dst, sem, i, step):
        part = pl.ds(i * step, step)
        return pltpu.make_async_copy(src.at[part], dst.at[part], sem.at[i])

    wk_copies = [piece(wk_hbm, wk, wk_sem, i, wk_step) for i in range(WK_PARTS)]
    kv_copies = [piece(kv_hbm, kv, kv_sem, i, kv_step) for i in range(CHUNKS)]
    wv_copies = [piece(wv_hbm, wv, wv_sem, i, wv_step) for i in range(WV_PARTS)]
    waiting = wk_copies + kv_copies + wv_copies
    for _ in range(WINDOW):
        waiting.pop(0).start()

    def arrive(copy):
        copy.wait()
        if waiting:
            waiting.pop(0).start()

    barrier = pltpu.get_barrier_semaphore()
    source_head = my_seq // per_shard
    own = source_head == my_head

    def greet(i):
        @pl.when(jnp.logical_not(jnp.logical_and(own, i == my_seq)))
        def _():
            pl.semaphore_signal(
                barrier, inc=1, device_id=(jnp.int32(i), source_head), device_id_type=MESH
            )

    loop(n_seq, greet)

    for copy in small:
        copy.wait()

    lane = lax.broadcasted_iota(jnp.int32, (batch, LANES), 1)
    request = lax.broadcasted_iota(jnp.int32, (batch, LANES), 0)
    length = jnp.zeros((batch, LANES), jnp.int32)
    for b in range(batch):
        length = jnp.where(request == b, len_ref[b], length)
    base = my_seq * (window * page_len)
    names = table[...]
    counts = jnp.zeros((batch, LANES), jnp.float32)
    for j in range(window):
        held = jnp.clip(length - (base + j * page_len), 0, page_len).astype(jnp.float32)
        counts = jnp.where(names[:, j : j + 1] == lane, held, counts)
    s_row = scale[...]
    s_hi = s_row.astype(jnp.bfloat16)
    s_rest = s_row - s_hi.astype(jnp.float32)
    s_mid = s_rest.astype(jnp.bfloat16)
    s_low = (s_rest - s_mid.astype(jnp.float32)).astype(jnp.bfloat16)
    per_page = jnp.concatenate(
        [counts[:, :pages]]
        + [s.astype(jnp.float32) for s in (s_hi, s_mid, s_low)]
        + [jnp.zeros((1, pages), jnp.float32)] * (8 - batch - 3),
        axis=0,
    ).astype(jnp.bfloat16)
    positions = pages * page_len
    spread = (
        lax.broadcasted_iota(jnp.int32, (pages, positions), 1) // page_len
        == lax.broadcasted_iota(jnp.int32, (pages, positions), 0)
    ).astype(jnp.float32).astype(jnp.bfloat16)
    per_pos = jnp.dot(per_page, spread, preferred_element_type=jnp.float32)
    scale_pos = per_pos[batch : batch + 1] + per_pos[batch + 1 : batch + 2] + per_pos[batch + 2 : batch + 3]

    query = qn[...].reshape(rows, nope).astype(jnp.float32)
    row_head = lax.broadcasted_iota(jnp.int32, (rows, nope), 0) % heads
    q_lat = jnp.zeros((rows, lat), jnp.float32)
    for i in range(WK_PARTS):
        wide = jnp.concatenate(
            [jnp.where(row_head == h, query, 0.0) for h in range(i * wk_step, (i + 1) * wk_step)],
            axis=1,
        ).astype(jnp.bfloat16)
        arrive(wk_copies[i])
        block = wk[pl.ds(i * wk_step, wk_step)].reshape(wk_step * nope, lat)
        q_lat = q_lat + jnp.dot(wide, block, preferred_element_type=jnp.float32)
    q_all = jnp.concatenate([q_lat.astype(jnp.bfloat16), qr[...].reshape(rows, rope)], axis=1)

    span = kv_step * page_len
    offset = (lax.broadcasted_iota(jnp.int32, (1, span), 1) % page_len).astype(jnp.float32)
    def scores(c):
        arrive(kv_copies[c])
        block = kv[pl.ds(c * kv_step, kv_step)].reshape(span, lat + rope)
        return lax.dot_general(
            q_all, block, (((1,), (1,)), ((), ())), preferred_element_type=jnp.float32
        )

    def attend(c, raw):
        s_pos = scale_pos[:, c * span : (c + 1) * span]
        score = raw * (s_pos * softmax_scale)
        score = jnp.concatenate(
            [
                jnp.where(
                    jnp.broadcast_to(offset, (heads, span))
                    < jnp.broadcast_to(per_pos[b : b + 1, c * span : (c + 1) * span], (heads, span)),
                    score[b * heads : (b + 1) * heads],
                    floor_score,
                )
                for b in range(batch)
            ],
            axis=0,
        )
        peak = jnp.maximum(jnp.max(score, axis=1, keepdims=True), floor_peak)
        weight = jnp.exp(score - peak)
        total = jnp.sum(weight, axis=1, keepdims=True)
        prob = (weight * s_pos).astype(jnp.bfloat16)
        values = kv[pl.ds(c * kv_step, kv_step), :, :lat].reshape(span, lat)
        acc = jnp.dot(prob, values, preferred_element_type=jnp.float32)
        return peak, total, acc

    parts = []
    raw = scores(0)
    for c in range(1, CHUNKS):
        following = scores(c)
        parts.append(attend(c - 1, raw))
        raw = following
    parts.append(attend(CHUNKS - 1, raw))
    peak = functools.reduce(jnp.maximum, [p[0] for p in parts])
    total = jnp.zeros((rows, 1), jnp.float32)
    acc = jnp.zeros((rows, lat), jnp.float32)
    for p, t, a in parts:
        factor = jnp.exp(p - peak)
        total = total + t * factor
        acc = acc + a * factor

    col = lax.broadcasted_iota(jnp.int32, (rows, LANES), 1)
    pair = jnp.where(col == 0, peak, jnp.where(col == 1, total, 0.0))
    pair = jnp.concatenate([pair, jnp.zeros((LANES - rows, LANES), jnp.float32)], axis=0)
    stat[...] = pair.T[0:2]

    n_dest = per_shard * n_head

    @pl.when(own)
    def _():
        pl.semaphore_wait(barrier, n_dest - 1)

    @pl.when(jnp.logical_not(own))
    def _():
        pl.semaphore_wait(barrier, n_dest)

    def target(k):
        part, request_of = k // n_head, k % n_head
        slot = request_of * (heads // per_msg) + (part * width) // (vdim * per_msg)
        return my_head * per_shard + part, request_of, slot

    def remote(n, k):
        seq_of, head_of, slot = target(k)
        return pltpu.make_async_remote_copy(
            src_ref=stat if n == 0 else msg.at[slot],
            dst_ref=stat_in.at[my_seq] if n == 0 else acc_in.at[my_seq],
            send_sem=send_sem.at[n, k],
            recv_sem=recv_sem.at[n, my_seq],
            device_id=(jnp.int32(seq_of), jnp.int32(head_of)),
            device_id_type=MESH,
        )

    def local(n, i, slot):
        return pltpu.make_async_copy(
            stat if n == 0 else msg.at[slot],
            stat_in.at[i] if n == 0 else acc_in.at[i],
            recv_sem.at[n, i],
        )

    def is_me(k):
        seq_of, head_of, _ = target(k)
        return jnp.logical_and(seq_of == my_seq, head_of == my_head)

    def send(n, k):
        @pl.when(jnp.logical_not(is_me(k)))
        def _():
            remote(n, k).start()

        @pl.when(is_me(k))
        def _():
            local(n, my_seq, target(k)[2]).start()

    loop(n_dest, functools.partial(send, 0))

    high = acc.astype(jnp.bfloat16)
    low = (acc - high.astype(jnp.float32)).astype(jnp.bfloat16)
    both = jnp.concatenate([high, low], axis=0)
    out_head = lax.broadcasted_iota(jnp.int32, (rows, vdim), 0) % heads
    carried = jnp.zeros((rows, vdim), jnp.float32)
    for h in range(0, heads, 2):
        if h % wv_step == 0:
            arrive(wv_copies[h // wv_step])
        y = jnp.dot(
            both, jnp.concatenate([wv[h], wv[h + 1]], axis=1), preferred_element_type=jnp.float32
        )
        y = y[:rows] + y[rows:]
        carried = jnp.where(out_head == h, y[:, :vdim], carried)
        carried = jnp.where(out_head == h + 1, y[:, vdim:], carried)
    msg[...] = carried.reshape(msg.shape)

    loop(n_dest, functools.partial(send, 1))

    loop(n_seq, lambda i: local(0, i, 0).wait())
    peaks, totals = stat_in[:, 0, :], stat_in[:, 1, :]
    factor = jnp.exp(peaks - jnp.max(peaks, axis=0, keepdims=True))
    denominator = jnp.sum(factor * totals, axis=0, keepdims=True)
    used = lax.broadcasted_iota(jnp.int32, (1, LANES), 1) < rows
    factor = factor / jnp.where(used, denominator, 1.0)
    if n_seq < LANES:
        factor = jnp.concatenate(
            [factor, jnp.zeros((LANES - n_seq, LANES), jnp.float32)], axis=0
        )
    mix[...] = factor.T.reshape(mix.shape)
    first = (my_seq % per_shard) * width
    weights = mix[my_head * (heads // per_msg) + first // (vdim * per_msg)]
    loop(n_seq, lambda i: local(1, i, 0).wait())
    result = jnp.zeros((per_msg, vdim), jnp.float32)
    for i in range(n_seq):
        result = result + weights[:, i : i + 1] * acc_in[i]
    if width >= vdim:
        for r in range(per_msg):
            out_ref[:, r * vdim : (r + 1) * vdim] = result[r : r + 1].astype(out_ref.dtype)
    else:
        picked = result[:, :width]
        for k in range(1, vdim // width):
            here = (my_seq % (vdim // width)) == k
            picked = jnp.where(here, result[:, k * width : (k + 1) * width], picked)
        out_ref[...] = picked.astype(out_ref.dtype)

    def sent(k):
        @pl.when(jnp.logical_not(is_me(k)))
        def _():
            for n in range(2):
                remote(n, k).wait_send()

    loop(n_dest, sent)


def solution(mesh):
    n_seq, n_head = mesh.shape["seq"], mesh.shape["head"]

    def shards(q_nope, q_rope, w_key_up, w_value_up, latent_cache, page_scale, block_table, lengths):
        batch, heads, _ = q_nope.shape
        vdim = w_value_up.shape[2]
        width = heads * n_head * vdim // n_seq
        per_msg = max(1, width // vdim)
        n_dest = (n_seq // n_head) * n_head
        assert batch == n_head and batch * heads <= LANES and n_seq % n_head == 0
        vmem = lambda a: pltpu.VMEM(a.shape, a.dtype)
        scale_row = page_scale.reshape(1, page_scale.shape[0])
        big = (q_nope, q_rope, w_key_up, w_value_up, latent_cache, scale_row, block_table)
        return pl.pallas_call(
            functools.partial(kernel, n_seq, n_head, width),
            out_shape=pltpu.VMEM((1, width), jnp.bfloat16),
            in_specs=[pl.BlockSpec(memory_space=pl.ANY)] * 8,
            out_specs=pl.BlockSpec(memory_space=pltpu.VMEM),
            scratch_shapes=[vmem(a) for a in big]
            + [
                pltpu.SMEM(lengths.shape, lengths.dtype),
                pltpu.VMEM((batch * heads // per_msg, per_msg, vdim), jnp.float32),
                pltpu.VMEM((2, LANES), jnp.float32),
                pltpu.VMEM((n_seq, per_msg, vdim), jnp.float32),
                pltpu.VMEM((n_seq, 2, LANES), jnp.float32),
                pltpu.VMEM((LANES // per_msg, per_msg, LANES), jnp.float32),
                pltpu.SemaphoreType.DMA((5,)),
                pltpu.SemaphoreType.DMA((WK_PARTS,)),
                pltpu.SemaphoreType.DMA((CHUNKS,)),
                pltpu.SemaphoreType.DMA((WV_PARTS,)),
                pltpu.SemaphoreType.DMA((2, n_dest)),
                pltpu.SemaphoreType.DMA((2, n_seq)),
            ],
            compiler_params=pltpu.CompilerParams(collective_id=0, has_side_effects=True),
        )(*big, lengths)

    in_specs = (
        P(None, "head", None),
        P(None, "head", None),
        P("head", None, None),
        P("head", None, None),
        P("seq", None, None),
        P("seq"),
        P(None, "seq"),
        P(),
    )
    out_specs = P("head", "seq")
    return jax.shard_map(shards, mesh=mesh, in_specs=in_specs, out_specs=out_specs, check_vma=False)
```

```python
import functools

import jax
import jax.numpy as jnp
from jax import lax
from jax.experimental import pallas as pl
from jax.experimental.pallas import tpu as pltpu
from jax.sharding import PartitionSpec as P

floor_score = -1e30
floor_peak = -1e29
LANES = 128
CHUNKS = 4
WV_PARTS = 1
WINDOW = 6
WK_PARTS = 4
MESH = pl.DeviceIdType.MESH


def loop(count, body):
    if count <= 16:
        for i in range(count):
            body(i)
    else:
        def step(i, carry):
            body(i)
            return carry
        lax.fori_loop(0, count, step, 0)


def kernel(
    n_seq, n_head, width,
    qn_hbm, qr_hbm, wk_hbm, wv_hbm, kv_hbm, scale_hbm, table_hbm, len_hbm,
    out_ref,
    qn, qr, wk, wv, kv, scale, table, len_ref,
    msg, stat, acc_in, stat_in, mix,
    small_sem, wk_sem, kv_sem, wv_sem, send_sem, recv_sem,
):
    batch, heads, nope = qn.shape
    rope = qr.shape[2]
    lat, vdim = wv.shape[1], wv.shape[2]
    pages, page_len, _ = kv.shape
    window = table.shape[1]
    rows = batch * heads
    per_msg = msg.shape[1]
    per_shard = n_seq // n_head
    softmax_scale = (nope + rope) ** (-0.5)
    my_seq = lax.axis_index("seq")
    my_head = lax.axis_index("head")

    small = [
        pltpu.make_async_copy(src, dst, small_sem.at[i])
        for i, (src, dst) in enumerate(
            ((qn_hbm, qn), (qr_hbm, qr), (scale_hbm, scale), (table_hbm, table), (len_hbm, len_ref))
        )
    ]
    for copy in small:
        copy.start()
    wk_step, kv_step, wv_step = heads // WK_PARTS, pages // CHUNKS, heads // WV_PARTS

    def piece(src, dst, sem, i, step):
        part = pl.ds(i * step, step)
        return pltpu.make_async_copy(src.at[part], dst.at[part], sem.at[i])

    wk_copies = [piece(wk_hbm, wk, wk_sem, i, wk_step) for i in range(WK_PARTS)]
    kv_copies = [piece(kv_hbm, kv, kv_sem, i, kv_step) for i in range(CHUNKS)]
    wv_copies = [piece(wv_hbm, wv, wv_sem, i, wv_step) for i in range(WV_PARTS)]
    waiting = wk_copies + kv_copies + wv_copies
    for _ in range(WINDOW):
        waiting.pop(0).start()

    def arrive(copy):
        copy.wait()
        if waiting:
            waiting.pop(0).start()

    barrier = pltpu.get_barrier_semaphore()
    source_head = my_seq // per_shard
    own = source_head == my_head

    def greet(i):
        @pl.when(jnp.logical_not(jnp.logical_and(own, i == my_seq)))
        def _():
            pl.semaphore_signal(
                barrier, inc=1, device_id=(jnp.int32(i), source_head), device_id_type=MESH
            )

    loop(n_seq, greet)

    for copy in small:
        copy.wait()

    lane = lax.broadcasted_iota(jnp.int32, (batch, LANES), 1)
    request = lax.broadcasted_iota(jnp.int32, (batch, LANES), 0)
    length = jnp.zeros((batch, LANES), jnp.int32)
    for b in range(batch):
        length = jnp.where(request == b, len_ref[b], length)
    base = my_seq * (window * page_len)
    names = table[...]
    counts = jnp.zeros((batch, LANES), jnp.float32)
    for j in range(window):
        held = jnp.clip(length - (base + j * page_len), 0, page_len).astype(jnp.float32)
        counts = jnp.where(names[:, j : j + 1] == lane, held, counts)
    s_row = scale[...]
    s_hi = s_row.astype(jnp.bfloat16)
    s_rest = s_row - s_hi.astype(jnp.float32)
    s_mid = s_rest.astype(jnp.bfloat16)
    s_low = (s_rest - s_mid.astype(jnp.float32)).astype(jnp.bfloat16)
    per_page = jnp.concatenate(
        [counts[:, :pages]]
        + [s.astype(jnp.float32) for s in (s_hi, s_mid, s_low)]
        + [jnp.zeros((1, pages), jnp.float32)] * (8 - batch - 3),
        axis=0,
    ).astype(jnp.bfloat16)
    positions = pages * page_len
    spread = (
        lax.broadcasted_iota(jnp.int32, (pages, positions), 1) // page_len
        == lax.broadcasted_iota(jnp.int32, (pages, positions), 0)
    ).astype(jnp.float32).astype(jnp.bfloat16)
    per_pos = jnp.dot(per_page, spread, preferred_element_type=jnp.float32)
    scale_pos = per_pos[batch : batch + 1] + per_pos[batch + 1 : batch + 2] + per_pos[batch + 2 : batch + 3]

    query = qn[...].reshape(rows, nope).astype(jnp.float32)
    row_head = lax.broadcasted_iota(jnp.int32, (rows, nope), 0) % heads
    q_lat = jnp.zeros((rows, lat), jnp.float32)
    for i in range(WK_PARTS):
        wide = jnp.concatenate(
            [jnp.where(row_head == h, query, 0.0) for h in range(i * wk_step, (i + 1) * wk_step)],
            axis=1,
        ).astype(jnp.bfloat16)
        arrive(wk_copies[i])
        block = wk[pl.ds(i * wk_step, wk_step)].reshape(wk_step * nope, lat)
        q_lat = q_lat + jnp.dot(wide, block, preferred_element_type=jnp.float32)
    q_all = jnp.concatenate([q_lat.astype(jnp.bfloat16), qr[...].reshape(rows, rope)], axis=1)

    span = kv_step * page_len
    offset = (lax.broadcasted_iota(jnp.int32, (1, span), 1) % page_len).astype(jnp.float32)
    def scores(c):
        arrive(kv_copies[c])
        block = kv[pl.ds(c * kv_step, kv_step)].reshape(span, lat + rope)
        return lax.dot_general(
            q_all, block, (((1,), (1,)), ((), ())), preferred_element_type=jnp.float32
        )

    def attend(c, raw):
        s_pos = scale_pos[:, c * span : (c + 1) * span]
        score = raw * (s_pos * softmax_scale)
        score = jnp.concatenate(
            [
                jnp.where(
                    jnp.broadcast_to(offset, (heads, span))
                    < jnp.broadcast_to(per_pos[b : b + 1, c * span : (c + 1) * span], (heads, span)),
                    score[b * heads : (b + 1) * heads],
                    floor_score,
                )
                for b in range(batch)
            ],
            axis=0,
        )
        peak = jnp.maximum(jnp.max(score, axis=1, keepdims=True), floor_peak)
        weight = jnp.exp(score - peak)
        total = jnp.sum(weight, axis=1, keepdims=True)
        prob = (weight * s_pos).astype(jnp.bfloat16)
        values = kv[pl.ds(c * kv_step, kv_step), :, :lat].reshape(span, lat)
        acc = jnp.dot(prob, values, preferred_element_type=jnp.float32)
        return peak, total, acc

    parts = []
    raw = scores(0)
    for c in range(1, CHUNKS):
        following = scores(c)
        parts.append(attend(c - 1, raw))
        raw = following
    parts.append(attend(CHUNKS - 1, raw))
    peak = functools.reduce(jnp.maximum, [p[0] for p in parts])
    total = jnp.zeros((rows, 1), jnp.float32)
    acc = jnp.zeros((rows, lat), jnp.float32)
    for p, t, a in parts:
        factor = jnp.exp(p - peak)
        total = total + t * factor
        acc = acc + a * factor

    col = lax.broadcasted_iota(jnp.int32, (rows, LANES), 1)
    pair = jnp.where(col == 0, peak, jnp.where(col == 1, total, 0.0))
    pair = jnp.concatenate([pair, jnp.zeros((LANES - rows, LANES), jnp.float32)], axis=0)
    stat[...] = pair.T[0:2]

    n_dest = per_shard * n_head

    @pl.when(own)
    def _():
        pl.semaphore_wait(barrier, n_dest - 1)

    @pl.when(jnp.logical_not(own))
    def _():
        pl.semaphore_wait(barrier, n_dest)

    def target(k):
        part, request_of = k // n_head, k % n_head
        slot = request_of * (heads // per_msg) + (part * width) // (vdim * per_msg)
        return my_head * per_shard + part, request_of, slot

    def remote(n, k):
        seq_of, head_of, slot = target(k)
        return pltpu.make_async_remote_copy(
            src_ref=stat if n == 0 else msg.at[slot],
            dst_ref=stat_in.at[my_seq] if n == 0 else acc_in.at[my_seq],
            send_sem=send_sem.at[n, k],
            recv_sem=recv_sem.at[n, my_seq],
            device_id=(jnp.int32(seq_of), jnp.int32(head_of)),
            device_id_type=MESH,
        )

    def local(n, i, slot):
        return pltpu.make_async_copy(
            stat if n == 0 else msg.at[slot],
            stat_in.at[i] if n == 0 else acc_in.at[i],
            recv_sem.at[n, i],
        )

    def is_me(k):
        seq_of, head_of, _ = target(k)
        return jnp.logical_and(seq_of == my_seq, head_of == my_head)

    def send(n, k):
        @pl.when(jnp.logical_not(is_me(k)))
        def _():
            remote(n, k).start()

        @pl.when(is_me(k))
        def _():
            local(n, my_seq, target(k)[2]).start()

    loop(n_dest, functools.partial(send, 0))

    high = acc.astype(jnp.bfloat16)
    low = (acc - high.astype(jnp.float32)).astype(jnp.bfloat16)
    both = jnp.concatenate([high, low], axis=0)
    out_head = lax.broadcasted_iota(jnp.int32, (rows, vdim), 0) % heads
    carried = jnp.zeros((rows, vdim), jnp.float32)
    for h in range(0, heads, 2):
        if h % wv_step == 0:
            arrive(wv_copies[h // wv_step])
        y = jnp.dot(
            both, jnp.concatenate([wv[h], wv[h + 1]], axis=1), preferred_element_type=jnp.float32
        )
        y = y[:rows] + y[rows:]
        carried = jnp.where(out_head == h, y[:, :vdim], carried)
        carried = jnp.where(out_head == h + 1, y[:, vdim:], carried)
    msg[...] = carried.reshape(msg.shape)

    loop(n_dest, functools.partial(send, 1))

    loop(n_seq, lambda i: local(0, i, 0).wait())
    peaks, totals = stat_in[:, 0, :], stat_in[:, 1, :]
    factor = jnp.exp(peaks - jnp.max(peaks, axis=0, keepdims=True))
    denominator = jnp.sum(factor * totals, axis=0, keepdims=True)
    used = lax.broadcasted_iota(jnp.int32, (1, LANES), 1) < rows
    factor = factor / jnp.where(used, denominator, 1.0)
    if n_seq < LANES:
        factor = jnp.concatenate(
            [factor, jnp.zeros((LANES - n_seq, LANES), jnp.float32)], axis=0
        )
    mix[...] = factor.T.reshape(mix.shape)
    first = (my_seq % per_shard) * width
    weights = mix[my_head * (heads // per_msg) + first // (vdim * per_msg)]
    loop(n_seq, lambda i: local(1, i, 0).wait())
    result = jnp.zeros((per_msg, vdim), jnp.float32)
    for i in range(n_seq):
        result = result + weights[:, i : i + 1] * acc_in[i]
    if width >= vdim:
        for r in range(per_msg):
            out_ref[:, r * vdim : (r + 1) * vdim] = result[r : r + 1].astype(out_ref.dtype)
    else:
        picked = result[:, :width]
        for k in range(1, vdim // width):
            here = (my_seq % (vdim // width)) == k
            picked = jnp.where(here, result[:, k * width : (k + 1) * width], picked)
        out_ref[...] = picked.astype(out_ref.dtype)

    def sent(k):
        @pl.when(jnp.logical_not(is_me(k)))
        def _():
            for n in range(2):
                remote(n, k).wait_send()

    loop(n_dest, sent)


def solution(mesh):
    n_seq, n_head = mesh.shape["seq"], mesh.shape["head"]

    def shards(q_nope, q_rope, w_key_up, w_value_up, latent_cache, page_scale, block_table, lengths):
        batch, heads, _ = q_nope.shape
        vdim = w_value_up.shape[2]
        width = heads * n_head * vdim // n_seq
        per_msg = max(1, width // vdim)
        n_dest = (n_seq // n_head) * n_head
        assert batch == n_head and batch * heads <= LANES and n_seq % n_head == 0
        vmem = lambda a: pltpu.VMEM(a.shape, a.dtype)
        scale_row = page_scale.reshape(1, page_scale.shape[0])
        big = (q_nope, q_rope, w_key_up, w_value_up, latent_cache, scale_row, block_table)
        return pl.pallas_call(
            functools.partial(kernel, n_seq, n_head, width),
            out_shape=pltpu.VMEM((1, width), jnp.bfloat16),
            in_specs=[pl.BlockSpec(memory_space=pl.ANY)] * 8,
            out_specs=pl.BlockSpec(memory_space=pltpu.VMEM),
            scratch_shapes=[vmem(a) for a in big]
            + [
                pltpu.SMEM(lengths.shape, lengths.dtype),
                pltpu.VMEM((batch * heads // per_msg, per_msg, vdim), jnp.float32),
                pltpu.VMEM((2, LANES), jnp.float32),
                pltpu.VMEM((n_seq, per_msg, vdim), jnp.float32),
                pltpu.VMEM((n_seq, 2, LANES), jnp.float32),
                pltpu.VMEM((LANES // per_msg, per_msg, LANES), jnp.float32),
                pltpu.SemaphoreType.DMA((5,)),
                pltpu.SemaphoreType.DMA((WK_PARTS,)),
                pltpu.SemaphoreType.DMA((CHUNKS,)),
                pltpu.SemaphoreType.DMA((WV_PARTS,)),
                pltpu.SemaphoreType.DMA((2, n_dest)),
                pltpu.SemaphoreType.DMA((2, n_seq)),
            ],
            compiler_params=pltpu.CompilerParams(collective_id=0, has_side_effects=True),
        )(*big, lengths)

    in_specs = (
        P(None, "head", None),
        P(None, "head", None),
        P("head", None, None),
        P("head", None, None),
        P("seq", None, None),
        P("seq"),
        P(None, "seq"),
        P(),
    )
    out_specs = P("head", "seq")
    return jax.shard_map(shards, mesh=mesh, in_specs=in_specs, out_specs=out_specs, check_vma=False)
```
